32 devices in a mesh: patch: 16 (over z, y, core), band: 2 (over x).
Axes of the slice: x: 2, y: 2, z: 4, core: 2. Of those that a mesh axis runs over, the one named last changes fastest.
Arguments:
- latents: float32 [10240, 512], P('patch', 'band'), may hold values from -6 to 6
- edge_latents: float32 [81920, 512], P(('patch', 'band')), may hold values from -6 to 6
- edge_sender: int32 [81920], P(('patch', 'band')), may hold values from 0 to 575, as said below
- edge_receiver: int32 [81920], P(('patch', 'band')), may hold values from 0 to 319
- block_counts: int32 [640], P(('patch', 'band')), may hold values from 16 to 128, as said below
- send_rows: int32 [32, 32, 8], P(('patch', 'band')), may hold values from 0 to 319
- edge_first_weight: bfloat16 [2, 1536, 512], replicated, may hold values from -0.15625 to 0.15625
- edge_first_bias: float32 [2, 512], replicated, may hold values from -3 to 3
- edge_second_weight: bfloat16 [2, 512, 512], replicated
- edge_gain: float32 [2, 512], replicated, may hold values from 0.1 to 1.9
- edge_offset: float32 [2, 512], replicated, may hold values from -3 to 3
- node_first_weight: bfloat16 [2, 1024, 512], replicated, may hold values from -0.1875 to 0.1875
- node_first_bias: float32 [2, 512], replicated, may hold values from -3 to 3
- node_second_weight: bfloat16 [2, 512, 512], replicated
- node_gain: float32 [2, 512], replicated, may hold values from 0.1 to 1.9
- node_offset: float32 [2, 512], replicated, may hold values from -3 to 3
Outputs:
- new_nodes: float32 [10240, 512], P(('patch', 'band'))
- new_edges: float32 [81920, 512], P(('patch', 'band'))
The draws below stay inside these ranges and needn't reach their ends.
Inputs may be any that keep to these rules, and one draw needn't show every extreme that they name: `edge_sender`: an entry below 320 names a node row of the edge's own device; an entry k above names slot (k - 320) % 8 of the rows that device (k - 320) // 8 sends to the edge's device. `block_counts`: the used slots of a block are its first ones; every device has a full block. send_rows[d, q] lists node rows of device d, numbered within d, that device q receives from d.
All inputs are finite; a program needn't handle non-finite values.
Results may differ from the reference program's by a relative error of at most 0.0045.
Values may be sent and summed in bfloat16 or wider, within the bound.
No kernel may reach another device: no remote copies, remote signals or barrier semaphores. Data moves between devices by JAX's collectives and lax.ppermute only.
A program may use at most 128 MiB of HBM per device.

```python
import math
import jax
import jax.numpy as jnp
from jax import lax

D = 512
HID = 512
NODE_DEV = 320
BLOCKS = 20
BLOCK = 128
SLOT = 8
LAYERS = 2
SHARDS = 32
NODES = 10240
EDGE_DEV = 2560
EDGES = 81920


def draw_edge_sender(key, part):
    subkeys = jax.random.split(jax.random.fold_in(key, 5), 6)
    shape_two = (SHARDS, EDGE_DEV)
    lower = SLOT // 2 + 1
    counts = lower + jax.random.randint(subkeys[0], (SHARDS, SHARDS), 0, 1 << 20) % (SLOT + 1 - lower)
    fullest = jax.random.randint(subkeys[1], (SHARDS, 1), 0, SHARDS)
    counts = jnp.where(jnp.arange(SHARDS)[None, :] == fullest, SLOT, counts)
    local_rows = jax.random.randint(subkeys[2], shape_two, 0, NODE_DEV)
    source_shard = jax.random.randint(subkeys[3], shape_two, 0, SHARDS)
    spread_bits = jax.random.randint(subkeys[4], shape_two, 0, 1 << 20)
    chosen = jnp.take_along_axis(counts, source_shard, axis=1)
    remote = NODE_DEV + source_shard * SLOT + spread_bits % chosen
    picker = jax.random.randint(subkeys[5], shape_two, 0, 2)
    return jnp.where(picker == 0, local_rows, remote).reshape(-1).astype(jnp.int32)


def draw_block_counts(key, part):
    subkeys = jax.random.split(jax.random.fold_in(key, 7), 3)
    floor_value = max(1, BLOCK // 8)
    device_low = jax.random.randint(subkeys[0], (SHARDS, 1), floor_value, BLOCK + 1)
    raw_bits = jax.random.randint(subkeys[1], (SHARDS, BLOCKS), 0, 1 << 20)
    counts = device_low + raw_bits % (BLOCK + 1 - device_low)
    full_block = jax.random.randint(subkeys[2], (SHARDS, 1), 0, BLOCKS)
    counts = jnp.where(jnp.arange(BLOCKS)[None, :] == full_block, BLOCK, counts)
    return counts.reshape(-1).astype(jnp.int32)


def scaled_weight(key, depth_count, fan_rows, fan_cols):
    subkeys = jax.random.split(key, 2)
    base = jax.random.normal(subkeys[0], (depth_count, fan_rows, fan_cols), jnp.float32)
    column_scale = jnp.exp(jax.random.uniform(subkeys[1], (depth_count, 1, fan_cols), jnp.float32, math.log(0.3), math.log(3.0)))
    return base * column_scale * fan_rows ** (-0.5)


def draw_edge_second_weight(key, part):
    return scaled_weight(jax.random.fold_in(key, 21), LAYERS, HID, D).astype(jnp.bfloat16)


def draw_node_second_weight(key, part):
    return scaled_weight(jax.random.fold_in(key, 23), LAYERS, HID, D).astype(jnp.bfloat16)


def with_ends(array, stream_key, low, top_value):
    longest = array.shape.index(max(array.shape))
    spots = []
    for shift in (0, 1):
        where = [jax.random.randint(jax.random.fold_in(stream_key, axis), (), 0, length) for axis, length in enumerate(array.shape)]
        where[longest] = (where[longest] + shift) % array.shape[longest]
        spots.append(tuple(where))
    return array.at[spots[0]].set(low).at[spots[1]].set(top_value)


def levels(own_key, shape, cuts, low, largest):
    loudness = 1.0
    for dim, parts in cuts:
        heights = jax.random.uniform(jax.random.fold_in(jax.random.fold_in(own_key, 6), dim), (parts,), jnp.float32, low / len(cuts), largest / len(cuts))
        loudness = loudness * jnp.repeat(jnp.exp(heights), shape[dim] // parts).reshape((-1,) + (1,) * (len(shape) - 1 - dim))
    return loudness


def gaussian(own_key, dims, scale, limit, cuts=(), kind=jnp.bfloat16):
    values = jax.random.normal(own_key, dims, jnp.float32) * scale
    if len(cuts) > 0:
        values = levels(own_key, dims, cuts, -0.22, 0.18) * values
    return jnp.clip(values, min=-limit, max=limit).astype(kind)


def setup_inputs(seed: int = 0) -> dict:
    arg_keys = jax.random.split(jax.random.key(seed), 17)
    latents = gaussian(arg_keys[0], (NODES, D), 1.0, 6.0, ((0, 16), (1, 2)), jnp.float32)
    edge_latents = gaussian(arg_keys[1], (EDGES, D), 1.0, 6.0, ((0, 32),), jnp.float32)
    edge_sender = draw_edge_sender(jax.random.fold_in(arg_keys[16], 71), 0)
    edge_receiver = with_ends(jax.random.randint(arg_keys[3], (EDGES,), 0, NODE_DEV), jax.random.fold_in(arg_keys[3], 1), 0, NODE_DEV - 1).astype(jnp.int32)
    block_counts = draw_block_counts(jax.random.fold_in(arg_keys[16], 71), 0)
    send_rows = with_ends(jax.random.randint(arg_keys[5], (SHARDS, SHARDS, SLOT), 0, NODE_DEV), jax.random.fold_in(arg_keys[5], 1), 0, NODE_DEV - 1).astype(jnp.int32)
    edge_first_weight = gaussian(arg_keys[6], (LAYERS, 3 * D, HID), (3 * D) ** -0.5, 0.15625)
    edge_first_bias = gaussian(arg_keys[7], (LAYERS, HID), 0.5, 3.0, (), jnp.float32)
    edge_second_weight = draw_edge_second_weight(jax.random.fold_in(arg_keys[16], 71), 0)
    edge_gain = jnp.clip(1.0 + 0.18 * jax.random.normal(arg_keys[9], (LAYERS, D), jnp.float32), 0.1, 1.9)
    edge_offset = gaussian(arg_keys[10], (LAYERS, D), 0.5, 3.0, (), jnp.float32)
    node_first_weight = gaussian(arg_keys[11], (LAYERS, 2 * D, HID), (2 * D) ** -0.5, 0.1875)
    node_first_bias = gaussian(arg_keys[12], (LAYERS, HID), 0.5, 3.0, (), jnp.float32)
    node_second_weight = draw_node_second_weight(jax.random.fold_in(arg_keys[16], 71), 0)
    node_gain = jnp.clip(1.0 + 0.18 * jax.random.normal(arg_keys[14], (LAYERS, D), jnp.float32), 0.1, 1.9)
    node_offset = gaussian(arg_keys[15], (LAYERS, D), 0.5, 3.0, (), jnp.float32)
    return {"latents": latents, "edge_latents": edge_latents, "edge_sender": edge_sender, "edge_receiver": edge_receiver, "block_counts": block_counts, "send_rows": send_rows, "edge_first_weight": edge_first_weight, "edge_first_bias": edge_first_bias, "edge_second_weight": edge_second_weight, "edge_gain": edge_gain, "edge_offset": edge_offset, "node_first_weight": node_first_weight, "node_first_bias": node_first_bias, "node_second_weight": node_second_weight, "node_gain": node_gain, "node_offset": node_offset}


epsilon = 1e-05

def layer_norm(values, norm_gain, norm_offset):
    centre = values - lax.optimization_barrier(jnp.mean(values, axis=-1, keepdims=True))
    spread = lax.optimization_barrier(jnp.mean(centre * centre, axis=-1, keepdims=True))
    return centre * lax.rsqrt(spread + epsilon) * norm_gain + norm_offset

def perceptron(pieces, first_weight, first_bias, second_weight, norm_gain, norm_offset):
    columns = pieces[0].shape[1]
    running = first_bias
    for position in range(len(pieces)):
        running = running + jnp.dot(pieces[position], first_weight[position * columns:(position + 1) * columns], preferred_element_type=jnp.float32)
    active = (running * jax.nn.sigmoid(running)).astype(jnp.bfloat16)
    result = jnp.dot(active, second_weight, preferred_element_type=jnp.float32)
    return layer_norm(result, norm_gain, norm_offset)

def reference(latents, edge_latents, edge_sender, edge_receiver, block_counts, send_rows, edge_first_weight, edge_first_bias, edge_second_weight, edge_gain, edge_offset, node_first_weight, node_first_bias, node_second_weight, node_gain, node_offset):
    shards = NODES // NODE_DEV
    slot_index = jnp.arange(EDGES, dtype=jnp.int32)
    owning = slot_index // EDGE_DEV
    beyond = edge_sender - NODE_DEV
    source_shard = jnp.clip(beyond // SLOT, 0, shards - 1).astype(jnp.int32)
    slot_pos = jnp.clip(beyond % SLOT, 0, SLOT - 1).astype(jnp.int32)
    remote = source_shard * NODE_DEV + send_rows[source_shard, owning, slot_pos]
    senders = jnp.where(edge_sender < NODE_DEV, owning * NODE_DEV + edge_sender, remote).astype(jnp.int32)
    receivers = (owning * NODE_DEV + edge_receiver).astype(jnp.int32)
    usable = slot_index % BLOCK < block_counts[slot_index // BLOCK]
    node_state = latents
    edge_state = edge_latents
    for layer_index in range(LAYERS):
        node_low = node_state.astype(jnp.bfloat16)

        def portion(operands):
            edge_part, send_part, recv_part = operands
            return perceptron((edge_part.astype(jnp.bfloat16), node_low[send_part], node_low[recv_part]), edge_first_weight[layer_index], edge_first_bias[layer_index], edge_second_weight[layer_index], edge_gain[layer_index], edge_offset[layer_index])
        update = lax.map(portion, (edge_state.reshape(shards, EDGE_DEV, D), senders.reshape(shards, EDGE_DEV), receivers.reshape(shards, EDGE_DEV)))
        update = update.reshape(EDGES, D)
        edge_state = edge_state + jnp.where(usable[:, None], update, jnp.zeros_like(update))
        edge_out_low = lax.optimization_barrier(edge_state.astype(jnp.bfloat16)).astype(jnp.float32)
        summed = jax.ops.segment_sum(jnp.where(usable[:, None], edge_out_low, jnp.zeros_like(edge_out_low)), receivers, num_segments=NODES)
        summed_low = summed.astype(jnp.bfloat16)
        node_state = node_state + perceptron((node_low, summed_low), node_first_weight[layer_index], node_first_bias[layer_index], node_second_weight[layer_index], node_gain[layer_index], node_offset[layer_index])
    return (node_state, edge_state)
```

```python
import functools

import jax
import jax.numpy as jnp
from jax import lax
from jax.experimental import pallas as pl
from jax.experimental.pallas import tpu as pltpu
from jax.sharding import PartitionSpec as P

epsilon = 1e-05
f32 = jnp.float32
bf16 = jnp.bfloat16
AXES = ("patch", "band")


def layer_norm(values, norm_gain, norm_offset):
    centre = values - jnp.mean(values, axis=-1, keepdims=True)
    spread = jnp.mean(centre * centre, axis=-1, keepdims=True)
    return centre * lax.rsqrt(spread + epsilon) * norm_gain + norm_offset


def swish(values):
    half = 0.5 * values
    return half * jnp.tanh(half) + half


def matmul(left, right):
    return jnp.dot(left, right, preferred_element_type=f32)


def column(row):
    return jnp.broadcast_to(row, (128, row.shape[1])).T[:, :1]


def one_hot(hits):
    return jnp.where(hits, 1.0, 0.0).astype(bf16)


def lanes(rows, columns):
    return lax.broadcasted_iota(jnp.int32, (rows, columns), 1)


def select_rows(send_ref, node_low):
    hits = column(send_ref[...]) == lanes(send_ref.shape[1], node_low.shape[0])
    return matmul(one_hot(hits), node_low).astype(bf16)


def start_kernel(band_ref, received_ref, latents_ref, send_ref, node_ref, outgoing_ref):
    bands, nodes, width = received_ref.shape
    band = band_ref[0]
    own = latents_ref[pl.ds(pl.multiple_of(band * nodes, 8), nodes), :]
    parts = [
        jnp.where(band == j, own, received_ref[j].astype(f32)) for j in range(bands)
    ]
    node_state = jnp.concatenate(parts, axis=1)
    node_ref[...] = node_state
    outgoing_ref[...] = select_rows(send_ref, node_state.astype(bf16))


def before_kernel(
    node_ref, edge_ref, sender_ref, receiver_ref, weight_ref, bias_ref, pre_ref, table_ref
):
    nodes, width = node_ref.shape

    @pl.when(pl.program_id(0) == 0)
    def _():
        node_low = node_ref[...].astype(bf16)
        for j in (0, 1):
            part = weight_ref[0, (1 + j) * width : (2 + j) * width, :]
            table_ref[j * nodes : (j + 1) * nodes, :] = matmul(node_low, part).astype(bf16)

    sender = sender_ref[0]
    rows = sender.shape[1]
    index = lanes(rows, 2 * nodes)
    local = column(jnp.where(sender < nodes, sender, -1))
    hits = (index == local) | (index == column(receiver_ref[0] + nodes))
    running = matmul(edge_ref[...].astype(bf16), weight_ref[0, :width, :])
    running = running + matmul(one_hot(hits), table_ref[...])
    pre_ref[...] = (running + bias_ref[0]).astype(bf16)


def after_kernel(
    count_ref,
    node_ref,
    incoming_ref,
    pre_ref,
    edge_ref,
    sender_ref,
    receiver_ref,
    first_ref,
    second_ref,
    gain_ref,
    offset_ref,
    node_bias_ref,
    node_gain_ref,
    node_offset_ref,
    send_ref,
    node_first_hbm,
    node_second_hbm,
    new_node_ref,
    new_edge_ref,
    outgoing_ref,
    table_ref,
    sum_ref,
    node_first_ref,
    node_second_ref,
    sems,
    *,
    layer,
    block_length,
):
    nodes, width = node_ref.shape
    step = pl.program_id(0)
    copies = (
        pltpu.make_async_copy(node_first_hbm.at[layer], node_first_ref, sems.at[0]),
        pltpu.make_async_copy(node_second_hbm.at[layer], node_second_ref, sems.at[1]),
    )

    @pl.when(step == 0)
    def _():
        for copy in copies:
            copy.start()
        table_ref[...] = matmul(incoming_ref[...], first_ref[0]).astype(bf16)
        sum_ref[...] = jnp.zeros_like(sum_ref)

    sender = sender_ref[0]
    rows = sender.shape[1]
    blocks = rows // block_length
    hits = column(sender - nodes) == lanes(rows, table_ref.shape[0])
    running = pre_ref[...].astype(f32) + matmul(one_hot(hits), table_ref[...])
    active = swish(running).astype(bf16)
    update = layer_norm(matmul(active, second_ref[0]), gain_ref[0], offset_ref[0])
    spot = lax.broadcasted_iota(jnp.int32, (block_length, 1), 0)
    place = lanes(1, block_length)
    receivers = []
    lows = []
    for j in range(blocks):
        part = slice(j * block_length, (j + 1) * block_length)
        count = count_ref[step * blocks + j]
        state = edge_ref[part, :] + jnp.where(spot < count, update[part], 0.0)
        new_edge_ref[part, :] = state
        lows.append(state.astype(bf16))
        receivers.append(jnp.where(place < count, receiver_ref[0, :, part], -1))
    receiver = jnp.concatenate(receivers, axis=1)
    low = jnp.concatenate(lows, axis=0)
    summing = one_hot(lax.broadcasted_iota(jnp.int32, (nodes, rows), 0) == receiver)
    sum_ref[...] += matmul(summing, low)

    @pl.when(step == pl.num_programs(0) - 1)
    def _():
        for copy in copies:
            copy.wait()
        node_state = node_ref[...]
        running = matmul(node_state.astype(bf16), node_first_ref[:width, :])
        running = running + matmul(sum_ref[...].astype(bf16), node_first_ref[width:, :])
        active = swish(running + node_bias_ref[0]).astype(bf16)
        result = matmul(active, node_second_ref[...])
        node_state = node_state + layer_norm(result, node_gain_ref[0], node_offset_ref[0])
        new_node_ref[...] = node_state
        outgoing_ref[...] = select_rows(send_ref, node_state.astype(bf16))


def whole(shape):
    return pl.BlockSpec(shape, lambda *_: (0,) * len(shape))


def of_layer(shape, layer, row=0):
    return pl.BlockSpec((1,) + shape, lambda *_: (layer, row, 0))


def shards(
    latents,
    edge_latents,
    edge_sender,
    edge_receiver,
    block_counts,
    send_rows,
    edge_first_weight,
    edge_first_bias,
    edge_second_weight,
    edge_gain,
    edge_offset,
    node_first_weight,
    node_first_bias,
    node_second_weight,
    node_gain,
    node_offset,
):
    layers = edge_first_weight.shape[0]
    edges, width = edge_latents.shape
    hidden = edge_first_weight.shape[2]
    bands = width // latents.shape[1]
    nodes = latents.shape[0] // bands
    halo = send_rows.shape[1] * send_rows.shape[2]
    block_length = edges // block_counts.shape[0]
    blocks = max(b for b in range(1, 5) if block_counts.shape[0] % b == 0)
    rows = blocks * block_length
    steps = edges // rows
    senders = edge_sender.reshape(steps, 1, rows)
    receivers = edge_receiver.reshape(steps, 1, rows)
    send_row = send_rows.reshape(1, halo)
    band = lax.axis_index("band").astype(jnp.int32).reshape(1)
    vectors = [
        v.reshape(layers, 1, -1)
        for v in (edge_first_bias, edge_gain, edge_offset, node_first_bias, node_gain, node_offset)
    ]
    first_bias, gain, offset, node_bias, n_gain, n_offset = vectors

    received = lax.all_to_all(
        latents.astype(bf16).reshape(bands, nodes, -1),
        "band", split_axis=0, concat_axis=0, tiled=True,
    )
    node_state, outgoing = pl.pallas_call(
        start_kernel,
        out_shape=(
            jax.ShapeDtypeStruct((nodes, width), f32),
            jax.ShapeDtypeStruct((halo, width), bf16),
        ),
        in_specs=[
            pl.BlockSpec(memory_space=pltpu.SMEM),
            whole(received.shape),
            whole(latents.shape),
            whole(send_row.shape),
        ],
        out_specs=(whole((nodes, width)), whole((halo, width))),
        grid=(1,),
        name="start",
    )(band, received, latents, send_row)

    edge_state = edge_latents
    row_block = pl.BlockSpec((rows, width), lambda s, *_: (s, 0))
    index_block = pl.BlockSpec((1, 1, rows), lambda s, *_: (s, 0, 0))
    for layer in range(layers):
        incoming = lax.all_to_all(
            outgoing.reshape(send_rows.shape[1], send_rows.shape[2], width),
            AXES, split_axis=0, concat_axis=0, tiled=True,
        ).reshape(halo, width)
        pre = pl.pallas_call(
            before_kernel,
            out_shape=jax.ShapeDtypeStruct((edges, hidden), bf16),
            grid=(steps,),
            in_specs=[
                whole((nodes, width)),
                row_block,
                index_block,
                index_block,
                of_layer((3 * width, hidden), layer),
                of_layer((1, hidden), layer),
            ],
            out_specs=pl.BlockSpec((rows, hidden), lambda s, *_: (s, 0)),
            scratch_shapes=[pltpu.VMEM((2 * nodes, hidden), bf16)],
            cost_estimate=pl.CostEstimate(
                flops=2 * edges * hidden * (width + 2 * nodes),
                bytes_accessed=edges * width * 6,
                transcendentals=0,
            ),
            name="before",
        )(node_state, edge_state, senders, receivers, edge_first_weight, first_bias)
        node_state, edge_state, outgoing = pl.pallas_call(
            functools.partial(after_kernel, layer=layer, block_length=block_length),
            out_shape=(
                jax.ShapeDtypeStruct((nodes, width), f32),
                jax.ShapeDtypeStruct((edges, width), f32),
                jax.ShapeDtypeStruct((halo, width), bf16),
            ),
            grid_spec=pltpu.PrefetchScalarGridSpec(
                num_scalar_prefetch=1,
                grid=(steps,),
                in_specs=[
                    whole((nodes, width)),
                    whole((halo, width)),
                    pl.BlockSpec((rows, hidden), lambda s, *_: (s, 0)),
                    row_block,
                    index_block,
                    index_block,
                    of_layer((width, hidden), layer, 1),
                    of_layer((hidden, width), layer),
                    of_layer((1, width), layer),
                    of_layer((1, width), layer),
                    of_layer((1, hidden), layer),
                    of_layer((1, width), layer),
                    of_layer((1, width), layer),
                    whole(send_row.shape),
                    pl.BlockSpec(memory_space=pl.ANY),
                    pl.BlockSpec(memory_space=pl.ANY),
                ],
                out_specs=(
                    whole((nodes, width)),
                    row_block,
                    whole((halo, width)),
                ),
                scratch_shapes=[
                    pltpu.VMEM((halo, hidden), bf16),
                    pltpu.VMEM((nodes, width), f32),
                    pltpu.VMEM(node_first_weight.shape[1:], bf16),
                    pltpu.VMEM(node_second_weight.shape[1:], bf16),
                    pltpu.SemaphoreType.DMA((2,)),
                ],
            ),
            name="after",
        )(
            block_counts,
            node_state,
            incoming,
            pre,
            edge_state,
            senders,
            receivers,
            edge_first_weight,
            edge_second_weight,
            gain,
            offset,
            node_bias,
            n_gain,
            n_offset,
            send_row,
            node_first_weight,
            node_second_weight,
        )
    return (node_state, edge_state)


def solution(mesh):
    split = P(AXES)
    return jax.shard_map(
        shards,
        mesh=mesh,
        in_specs=(
            P("patch", "band"),
            P(AXES, None),
            split,
            split,
            split,
            P(AXES, None, None),
        )
        + (P(),) * 10,
        out_specs=(P(AXES, None), P(AXES, None)),
        check_vma=False,
    )
```

```python
import functools

import jax
import jax.numpy as jnp
from jax import lax
from jax.experimental import pallas as pl
from jax.experimental.pallas import tpu as pltpu
from jax.sharding import PartitionSpec as P

epsilon = 1e-05
f32 = jnp.float32
bf16 = jnp.bfloat16
AXES = ("patch", "band")
STEP = 5
CHUNK = 5
LIMIT = 32 * 1024 * 1024


def layer_norm(values, norm_gain, norm_offset):
    centre = values - jnp.mean(values, axis=-1, keepdims=True)
    spread = jnp.mean(centre * centre, axis=-1, keepdims=True)
    return centre * lax.rsqrt(spread + epsilon) * norm_gain + norm_offset


def swish(values):
    half = 0.5 * values
    return half * jnp.tanh(half) + half


def matmul(left, right):
    return jnp.dot(left, right, preferred_element_type=f32)


def column(row):
    return jnp.broadcast_to(row, (128, row.shape[1])).T[:, :1]


def one_hot(hits):
    return jnp.where(hits, 1.0, 0.0).astype(bf16)


def lanes(rows, columns):
    return lax.broadcasted_iota(jnp.int32, (rows, columns), 1)


def select_rows(send_ref, node_low):
    hits = column(send_ref[...]) == lanes(send_ref.shape[1], node_low.shape[0])
    return matmul(one_hot(hits), node_low).astype(bf16)


def start_kernel(band_ref, received_ref, latents_ref, send_ref, node_ref, outgoing_ref):
    bands, nodes, width = received_ref.shape
    band = band_ref[0]
    own = latents_ref[pl.ds(pl.multiple_of(band * nodes, 8), nodes), :]
    parts = [
        jnp.where(band == j, own, received_ref[j].astype(f32)) for j in range(bands)
    ]
    node_state = jnp.concatenate(parts, axis=1)
    node_ref[...] = node_state
    outgoing_ref[...] = select_rows(send_ref, node_state.astype(bf16))


def before_kernel(
    node_ref, edge_ref, sender_ref, receiver_ref, weight_ref, bias_ref, pre_ref, table_ref, *, layer, chunk
):
    nodes, width = node_ref.shape

    @pl.when(pl.program_id(0) == 0)
    def _():
        node_low = node_ref[...].astype(bf16)
        for j in (0, 1):
            part = weight_ref[0, (1 + j) * width : (2 + j) * width, :]
            table_ref[j * nodes : (j + 1) * nodes, :] = matmul(node_low, part).astype(bf16)

    index = lanes(chunk, 2 * nodes)
    rows = sender_ref.shape[2]
    base = pl.multiple_of(pl.program_id(0) * rows, rows)
    for start in range(0, rows, chunk):
        part = slice(start, start + chunk)
        at = pl.ds(base + start, chunk)
        edge = edge_ref[part, :]
        sender = sender_ref[0, :, part]
        local = column(jnp.where(sender < nodes, sender, -1))
        hits = (index == local) | (index == column(receiver_ref[0, :, part] + nodes))
        running = matmul(edge.astype(bf16), weight_ref[0, :width, :])
        running = running + matmul(one_hot(hits), table_ref[...])
        pre_ref[at, :] = (running + bias_ref[layer : layer + 1, :]).astype(bf16)


def after_kernel(
    count_ref,
    node_ref,
    incoming_ref,
    pre_ref,
    edge_ref,
    sender_ref,
    receiver_ref,
    first_ref,
    second_ref,
    gain_ref,
    offset_ref,
    node_bias_ref,
    node_gain_ref,
    node_offset_ref,
    send_ref,
    node_first_hbm,
    node_second_hbm,
    new_node_ref,
    new_edge_ref,
    outgoing_ref,
    table_ref,
    sum_ref,
    node_first_ref,
    node_second_ref,
    sems,
    *,
    layer,
    block_length,
    chunk,
):
    nodes, width = node_ref.shape
    step = pl.program_id(0)
    copies = (
        pltpu.make_async_copy(node_first_hbm.at[layer], node_first_ref, sems.at[0]),
        pltpu.make_async_copy(node_second_hbm.at[layer], node_second_ref, sems.at[1]),
    )

    @pl.when(step == 0)
    def _():
        for copy in copies:
            copy.start()
        table_ref[...] = matmul(incoming_ref[...], first_ref[0]).astype(bf16)
        sum_ref[...] = jnp.zeros_like(sum_ref)

    rows = sender_ref.shape[2]
    base = pl.multiple_of(step * rows, rows)
    blocks = rows // block_length
    spot = lax.broadcasted_iota(jnp.int32, (block_length, 1), 0)
    place = lanes(1, block_length)
    gain = gain_ref[layer : layer + 1, :]
    offset = offset_ref[layer : layer + 1, :]
    for start in range(0, rows, chunk):
        part = slice(start, start + chunk)
        hits = column(sender_ref[0, :, part] - nodes) == lanes(chunk, table_ref.shape[0])
        running = pre_ref[pl.ds(base + start, chunk), :].astype(f32) + matmul(one_hot(hits), table_ref[...])
        active = swish(running).astype(bf16)
        update = layer_norm(matmul(active, second_ref[0]), gain, offset)
        receivers = []
        lows = []
        for inner in range(0, chunk, block_length):
            at = slice(start + inner, start + inner + block_length)
            count = count_ref[step * blocks + (start + inner) // block_length]
            change = jnp.where(spot < count, update[inner : inner + block_length], 0.0)
            state = edge_ref[at, :] + change
            new_edge_ref[at, :] = state
            lows.append(state.astype(bf16))
            receivers.append(jnp.where(place < count, receiver_ref[0, :, at], -1))
        receiver = jnp.concatenate(receivers, axis=1)
        low = jnp.concatenate(lows, axis=0)
        summing = one_hot(lax.broadcasted_iota(jnp.int32, (nodes, chunk), 0) == receiver)
        sum_ref[...] += matmul(summing, low)

    @pl.when(step == pl.num_programs(0) - 1)
    def _():
        for copy in copies:
            copy.wait()
        node_state = node_ref[...]
        running = matmul(node_state.astype(bf16), node_first_ref[:width, :])
        running = running + matmul(sum_ref[...].astype(bf16), node_first_ref[width:, :])
        active = swish(running + node_bias_ref[layer : layer + 1, :]).astype(bf16)
        result = matmul(active, node_second_ref[...])
        node_state = node_state + layer_norm(result, node_gain_ref[layer : layer + 1, :], node_offset_ref[layer : layer + 1, :])
        new_node_ref[...] = node_state
        outgoing_ref[...] = select_rows(send_ref, node_state.astype(bf16))


def in_hbm(*arrays):
    return tuple(pltpu.with_memory_space_constraint(a, pltpu.HBM) for a in arrays)


def largest(total, limit):
    return max(b for b in range(1, limit + 1) if total % b == 0)


def whole(shape):
    return pl.BlockSpec(shape, lambda *_: (0,) * len(shape))


def of_layer(shape, layer, row=0):
    return pl.BlockSpec((1,) + shape, lambda *_: (layer, row, 0))


def shards(
    latents,
    edge_latents,
    edge_sender,
    edge_receiver,
    block_counts,
    send_rows,
    edge_first_weight,
    edge_first_bias,
    edge_second_weight,
    edge_gain,
    edge_offset,
    node_first_weight,
    node_first_bias,
    node_second_weight,
    node_gain,
    node_offset,
):
    edge_first_weight, edge_first_bias, edge_second_weight, edge_gain, edge_offset = in_hbm(
        edge_first_weight, edge_first_bias, edge_second_weight, edge_gain, edge_offset
    )
    node_first_weight, node_first_bias, node_second_weight, node_gain, node_offset = in_hbm(
        node_first_weight, node_first_bias, node_second_weight, node_gain, node_offset
    )
    (own_latents,) = in_hbm(latents)
    layers = edge_first_weight.shape[0]
    edges, width = edge_latents.shape
    hidden = edge_first_weight.shape[2]
    bands = width // latents.shape[1]
    nodes = latents.shape[0] // bands
    halo = send_rows.shape[1] * send_rows.shape[2]
    block_length = edges // block_counts.shape[0]
    blocks = largest(block_counts.shape[0], STEP)
    rows = blocks * block_length
    chunk = largest(rows // block_length, CHUNK) * block_length
    steps = edges // rows
    senders = edge_sender.reshape(steps, 1, rows)
    receivers = edge_receiver.reshape(steps, 1, rows)
    send_row = send_rows.reshape(1, halo)
    senders, receivers, send_row = in_hbm(senders, receivers, send_row)
    band = lax.axis_index("band").astype(jnp.int32).reshape(1)
    received = lax.all_to_all(
        latents.astype(bf16).reshape(bands, nodes, -1),
        "band", split_axis=0, concat_axis=0, tiled=True,
    )
    node_state, outgoing = pl.pallas_call(
        start_kernel,
        out_shape=(
            pltpu.HBM((nodes, width), f32),
            pltpu.HBM((halo, width), bf16),
        ),
        in_specs=[
            pl.BlockSpec(memory_space=pltpu.SMEM),
            whole(received.shape),
            whole(latents.shape),
            whole(send_row.shape),
        ],
        out_specs=(whole((nodes, width)), whole((halo, width))),
        grid=(1,),
        compiler_params=pltpu.CompilerParams(vmem_limit_bytes=LIMIT),
        name="start",
    )(band, received, own_latents, send_row)

    edge_state = edge_latents
    resident = pl.BlockSpec(memory_space=pltpu.VMEM)
    row_block = pl.BlockSpec((rows, width), lambda s, *_: (s, 0))
    index_block = pl.BlockSpec((1, 1, rows), lambda s, *_: (s, 0, 0))
    for layer in range(layers):
        incoming = lax.all_to_all(
            jnp.reshape(outgoing, (send_rows.shape[1], send_rows.shape[2], width)),
            AXES, split_axis=0, concat_axis=0, tiled=True,
        ).reshape(halo, width)
        (node_state,) = in_hbm(node_state)
        (edge_state,) = in_hbm(edge_state)
        pre = pl.pallas_call(
            functools.partial(before_kernel, layer=layer, chunk=chunk),
            out_shape=pltpu.VMEM((edges, hidden), bf16),
            grid=(steps,),
            in_specs=[
                whole((nodes, width)),
                row_block,
                index_block,
                index_block,
                of_layer((3 * width, hidden), layer),
                whole((layers, width)),
            ],
            out_specs=resident,
            compiler_params=pltpu.CompilerParams(vmem_limit_bytes=LIMIT),
            scratch_shapes=[pltpu.VMEM((2 * nodes, hidden), bf16)],
            cost_estimate=pl.CostEstimate(
                flops=2 * edges * hidden * (width + 2 * nodes),
                bytes_accessed=edges * width * 6,
                transcendentals=0,
            ),
            name="before",
        )(node_state, edge_state, senders, receivers, edge_first_weight, edge_first_bias)
        node_state, edge_state, outgoing = pl.pallas_call(
            functools.partial(after_kernel, layer=layer, block_length=block_length, chunk=chunk),
            out_shape=(
                pltpu.HBM((nodes, width), f32),
                pltpu.HBM((edges, width), f32),
                pltpu.HBM((halo, width), bf16),
            ),
            grid_spec=pltpu.PrefetchScalarGridSpec(
                num_scalar_prefetch=1,
                grid=(steps,),
                in_specs=[
                    whole((nodes, width)),
                    whole((halo, width)),
                    resident,
                    row_block,
                    index_block,
                    index_block,
                    of_layer((width, hidden), layer, 1),
                    of_layer((hidden, width), layer),
                    whole((layers, width)),
                    whole((layers, width)),
                    whole((layers, width)),
                    whole((layers, width)),
                    whole((layers, width)),
                    whole(send_row.shape),
                    pl.BlockSpec(memory_space=pl.ANY),
                    pl.BlockSpec(memory_space=pl.ANY),
                ],
                out_specs=(
                    whole((nodes, width)),
                    row_block,
                    whole((halo, width)),
                ),
                scratch_shapes=[
                    pltpu.VMEM((halo, hidden), bf16),
                    pltpu.VMEM((nodes, width), f32),
                    pltpu.VMEM(node_first_weight.shape[1:], bf16),
                    pltpu.VMEM(node_second_weight.shape[1:], bf16),
                    pltpu.SemaphoreType.DMA((2,)),
                ],
            ),
            compiler_params=pltpu.CompilerParams(vmem_limit_bytes=LIMIT),
            name="after",
        )(
            block_counts,
            node_state,
            incoming,
            pre,
            edge_state,
            senders,
            receivers,
            edge_first_weight,
            edge_second_weight,
            edge_gain,
            edge_offset,
            node_first_bias,
            node_gain,
            node_offset,
            send_row,
            node_first_weight,
            node_second_weight,
        )
    return (node_state, edge_state)


def solution(mesh):
    split = P(AXES)
    return jax.shard_map(
        shards,
        mesh=mesh,
        in_specs=(
            P("patch", "band"),
            P(AXES, None),
            split,
            split,
            split,
            P(AXES, None, None),
        )
        + (P(),) * 10,
        out_specs=(P(AXES, None), P(AXES, None)),
        check_vma=False,
    )
```
